32 devices in a mesh: dp: 4 (over y, x), expert: 8 (over z, core).
Axes of the slice: x: 2, y: 2, z: 4, core: 2. Of those that a mesh axis runs over, the one named last changes fastest.
Arguments:
- expert_ids: int32 [1024, 4], P(('dp', 'expert')), may hold values from 0 to 7, all different within a row; in each aligned block of 32 rows (0 to 31, 32 to 63, ...) at most 20 rows name the same one
- expert_home: int32 [8], replicated, may hold values from 0 to 7, each once
- live_tokens: int32 [32], P(('dp', 'expert')), may hold values from 1 to 32, 768 in all
- gate_weights: float32 [1024, 4], P(('dp', 'expert')), may hold values from 0.1 to 1
- output_grad: bfloat16 [1024, 7168], P(('dp', 'expert')), may hold values from -6 to 6
- saved_hidden: bfloat16 [1024, 4, 1024], P(('dp', 'expert')), may hold values from -0.59765625 to 0.59765625
- down_weight: bfloat16 [8, 1024, 7168], P('expert'), may hold values from -0.1875 to 0.1875
- dense_input: bfloat16 [1024, 7168], P(('dp', 'expert')), may hold values from -6 to 6
- latent_grad: bfloat16 [1024, 256], P(('dp', 'expert')), may hold values from -0.1875 to 0.1875
Outputs:
- hidden_grad: bfloat16 [1024, 4, 1024], P(('dp', 'expert'))
- expert_grad: float32 [8, 1024, 7168], P('expert', 'dp')
- dense_grad: float32 [7168, 256], P(('dp', 'expert'))
The draws below stay inside these ranges and needn't reach their ends.
Inputs may be any that keep to these rules, and one draw needn't show every extreme that they name: `expert_ids`: each row names 4 different experts. Among the rows of one device no expert is named more than 20 times, and on some devices one expert is named exactly 20 times. A permutation: expert e is held at index expert_home[e] of the expert axis, in every dp replica. `live_tokens`: entry i is the number of real tokens at the start of device i, in the order of the joined dp and expert axes; the rest are padding. Some device has all 32 real.
All inputs are finite; a program needn't handle non-finite values.
Results may differ from the reference program's by a relative error of at most 0.008.
Values may be sent and summed in bfloat16 or wider, within the bound.
No kernel may reach another device: no remote copies, remote signals or barrier semaphores. Data moves between devices by JAX's collectives and lax.ppermute only.
A program may use at most 192 MiB of HBM per device.

```python
import math
import jax
import jax.numpy as jnp
import numpy as np
from jax import lax

D = 7168
KVR = 256
FFE = 1024
TOK_DEV = 32
EXPERTS = 8
TOPK = 4
CAP = 20
TOKENS = 1024
N_DP = 4
DEVICES = 32


def strengthened(result, own_key, source, target, shards_of, factor):
    owner, partner = [(jnp.arange(result.shape[position]) // (result.shape[position] // shards_of)).reshape([-1 if axis == position else 1 for axis in range(result.ndim)]) for position in (source, target)]
    chosen = jax.random.permutation(own_key, shards_of)[partner]
    strong = (owner == chosen) | (owner == (partner + shards_of // 2) % shards_of)
    return jnp.where(strong, factor * result, result)


def level_of(key, shape, split, low, top_value):
    gain = 1.0
    for dim, blocks in split:
        heights = jax.random.uniform(jax.random.fold_in(jax.random.fold_in(key, 6), dim), (blocks,), jnp.float32, low / len(split), top_value / len(split))
        gain = gain * jnp.repeat(jnp.exp(heights), shape[dim] // blocks).reshape((-1,) + (1,) * (len(shape) - 1 - dim))
    return gain


def profile(count, total, bound, skew):
    loads = [(1 << 20) // math.isqrt(standing ** skew) + 1 for standing in range(2, count + 1)]
    rest, given = total - bound - (count - 1), [1] * (count - 1)
    while rest > 0:
        movable = [i for i in range(count - 1) if given[i] < bound]
        mass, left = sum([loads[i] for i in movable]), rest
        for i in movable:
            addition = min(bound - given[i], max(1, left * loads[i] // mass), rest)
            given[i] = given[i] + addition
            rest = rest - addition
    return np.array([bound] + given)


def uneven(rng, amount, total, reach, lean):
    if amount == 2:
        one = jax.random.randint(rng, (), max(1, total - reach), min(reach, total - 1) + 1)
        return jnp.stack([one, total - one])
    sizes = jnp.asarray(profile(amount, total, reach, lean), jnp.int32)
    pairs = (amount - 1) // 2
    source_of, taker = sizes[1:1 + 2 * pairs:2], sizes[2:2 + 2 * pairs:2]
    room = jnp.minimum(source_of - 1, reach - taker)
    shifted = jax.random.randint(jax.random.fold_in(rng, 1), (pairs,), 0, 1 << 20) % (room + 1)
    sizes = sizes.at[1:1 + 2 * pairs:2].set(source_of - shifted).at[2:2 + 2 * pairs:2].set(taker + shifted)
    return sizes[jax.random.permutation(jax.random.fold_in(rng, 2), amount)]


def assign_block(own_key, own, number, rows, amount, top, limit, slope):
    ranking = jax.random.permutation(own_key, amount)
    crowded, ordinary = portions_of(amount, rows * top, limit, slope, True), portions_of(amount, rows * top, limit, slope, False)
    places = jnp.arange(amount)

    def named(lengths, turn):
        used = int((lengths > 0).sum())
        fixed = max(1, used // 4)
        shifted = fixed + (places - fixed + turn * (used - fixed)) % max(1, amount - fixed)
        return jnp.zeros((amount,), jnp.int32).at[ranking[jnp.where(places < fixed, places, shifted)]].set(jnp.asarray(lengths, jnp.int32))

    lengths = jnp.where(number % 4 == 0, named(crowded, number // 4), named(ordinary, number - number // 4 - 1))
    mixed = jax.random.permutation(jax.random.fold_in(own, 3), amount)
    giver, receiver = mixed[0:amount // 2 * 2:2], mixed[1:amount // 2 * 2:2]
    margin = jnp.minimum(lengths[giver] - 1, limit - lengths[receiver]) // 2
    margin = jnp.where((giver == ranking[0]) | (receiver == ranking[0]) | (lengths[receiver] == 0), 0, jnp.maximum(margin, 0))
    shifted = jax.random.randint(jax.random.fold_in(own, 4), (amount // 2,), 0, 1 << 20) % (margin + 1)
    lengths = lengths.at[giver].add(-shifted).at[receiver].add(shifted)
    items = jnp.searchsorted(jnp.cumsum(lengths), jnp.arange(rows * top), side="right").astype(jnp.int32)
    grid = items.reshape(top, rows).T
    grid = grid[jax.random.permutation(jax.random.fold_in(own, 1), rows)]
    turn = jax.random.randint(jax.random.fold_in(own, 2), (rows, 1), 0, top)
    return jnp.take_along_axis(grid, (jnp.arange(top)[None, :] + turn) % top, axis=1)


def portions_of(count, total, reach, slope, full):
    portions = [(1 << 20) // math.isqrt(grade ** slope) + 1 for grade in range(1, count + 1)]
    largest = reach if full else min(reach, max(-(-total // count), total * portions[0] // sum(portions)))
    least = 1 if total - largest >= count - 1 else 0
    holding, spare = [largest] + [least] * (count - 1), total - largest - least * (count - 1)
    while spare > 0:
        candidates = [i for i in range(1, count) if holding[i] < largest] or [i for i in range(1, count) if holding[i] < reach]
        mass, budget = sum([portions[i] for i in candidates]), spare
        for i in candidates:
            extra = min(reach - holding[i], max(1, budget * portions[i] // mass), spare)
            holding[i] = holding[i] + extra
            spare = spare - extra
    return np.array(holding)


def centred(own_key, dims, spread, reach, split=(), kind=jnp.bfloat16):
    drawn = spread * jax.random.normal(own_key, dims, jnp.float32)
    if split:
        drawn = drawn * level_of(own_key, dims, split, -0.22, 0.18)
    return jnp.clip(drawn, -reach, reach).astype(kind)


def gaussian_with(key, extent, width, bound, split, heavy, kind=jnp.bfloat16):
    array = width * jax.random.normal(key, extent, jnp.float32)
    if split:
        array = array * level_of(key, extent, split, -0.22, 0.18)
    return jnp.clip(strengthened(array, jax.random.fold_in(key, 3), *heavy), -bound, bound).astype(kind)


def setup_inputs(seed: int = 0) -> dict:
    seeds = jax.random.split(jax.random.key(seed), 10)
    expert_ids_keys = jax.random.split(jax.random.fold_in(seeds[0], 1), TOKENS // TOK_DEV)
    expert_ids_turns = jax.random.permutation(jax.random.fold_in(seeds[0], 3), TOKENS // TOK_DEV)
    expert_ids = jax.vmap(lambda own, number: assign_block(jax.random.fold_in(seeds[0], 2), own, number, TOK_DEV, EXPERTS, TOPK, CAP, 2))(expert_ids_keys, expert_ids_turns).reshape((TOKENS, TOPK))
    expert_home = jax.random.permutation(seeds[1], EXPERTS).astype(jnp.int32)
    live_tokens = uneven(seeds[2], DEVICES, DEVICES * TOK_DEV * 3 // 4, TOK_DEV, 2).astype(jnp.int32)
    gate_weights = jnp.clip(0.1 + 0.9 * jax.random.uniform(seeds[3], (TOKENS, TOPK), jnp.float32) ** level_of(seeds[3], (TOKENS, TOPK), ((0, 32),), -0.2, 0.2), 0.1, 1.0)
    output_grad = centred(seeds[4], (TOKENS, D), 0.5, 6.0, ((0, 32),))
    saved_hidden = gaussian_with(seeds[5], (TOKENS, TOPK, FFE), 0.1, 0.59765625, ((0, 32),), (0, 2, 32, 2.75))
    down_weight = centred(seeds[6], (EXPERTS, FFE, D), FFE ** -0.5, 0.1875, ((0, 8),))
    dense_input = gaussian_with(seeds[7], (TOKENS, D), 1.0, 6.0, ((0, 32),), (0, 1, 32, 2.75))
    latent_grad = centred(seeds[8], (TOKENS, KVR), TOKENS ** -0.5, 0.1875, ((0, 32),))
    return {"expert_ids": expert_ids, "expert_home": expert_home, "live_tokens": live_tokens, "gate_weights": gate_weights, "output_grad": output_grad, "saved_hidden": saved_hidden, "down_weight": down_weight, "dense_input": dense_input, "latent_grad": latent_grad}


def reference(expert_ids, expert_home, live_tokens, gate_weights, output_grad, saved_hidden, down_weight, dense_input, latent_grad):
    token_index = jnp.arange(TOK_DEV, dtype=jnp.int32)
    is_live = (token_index[None, :] < live_tokens[:, None]).reshape(TOKENS)
    masked_grad = jnp.where(is_live[:, None], latent_grad, jnp.zeros_like(latent_grad))
    dense_grad = jnp.dot(dense_input.T, masked_grad, preferred_element_type=jnp.float32)
    pair_home = expert_home[expert_ids]
    pair_scale = gate_weights * is_live[:, None].astype(jnp.float32)
    grad_wide = output_grad.astype(jnp.float32)

    def one_expert(carry, slot):
        chosen = pair_home == slot
        coefficient = jnp.sum(jnp.where(chosen, pair_scale, jnp.float32(0.0)), axis=1)
        gated = (grad_wide * coefficient[:, None]).astype(jnp.bfloat16)
        hidden_rows = jnp.sum(jnp.where(chosen[:, :, None], saved_hidden.astype(jnp.float32), jnp.float32(0.0)), axis=1)
        expert_weight = down_weight[slot]
        input_grad = jnp.dot(gated, expert_weight.T, preferred_element_type=jnp.float32).astype(jnp.bfloat16)
        carry = jnp.where(chosen[:, :, None], input_grad[:, None, :], carry)
        replica_hidden = hidden_rows.reshape(N_DP, TOKENS // N_DP, FFE)
        replica_grad = gated.astype(jnp.float32).reshape(N_DP, TOKENS // N_DP, D)
        partial_value = jnp.einsum("rtf,rtd->rfd", replica_hidden, replica_grad)
        summed = jnp.sum(partial_value, axis=0)
        return carry, summed

    start_grad = jnp.zeros((TOKENS, TOPK, FFE), jnp.bfloat16)
    hidden_grad, expert_grad = lax.scan(one_expert, start_grad, jnp.arange(EXPERTS, dtype=jnp.int32))
    return hidden_grad, expert_grad, dense_grad
```

```python
import jax
import jax.numpy as jnp
from jax import lax
from jax.sharding import PartitionSpec as P

ALL = ("dp", "expert")


class Torus:
    def __init__(self, n_dp, n_group):
        n_x = 2 if n_dp % 2 == 0 else 1
        self.n_core = 2
        self.shape = (n_dp // n_x, n_x, n_group // self.n_core)
        self.n_dev = n_dp * n_group
        self.n_group = n_group

    def coords(self, d):
        dp, e = divmod(d, self.n_group)
        y, x = divmod(dp, self.shape[1])
        z, core = divmod(e, self.n_core)
        return [y, x, z, core]

    def index(self, c):
        return ((c[0] * self.shape[1] + c[1]) * self.shape[2] + c[2]) * self.n_core + c[3]

    def fetch(self, piece, axis, step):
        rows, labels = piece
        size = self.shape[axis]
        pairs = []
        for d in range(self.n_dev):
            c = self.coords(d)
            c[axis] = (c[axis] - step) % size
            pairs.append((d, self.index(c)))
        moved = [
            tuple((v + step) % size if i == axis else v for i, v in enumerate(label))
            for label in labels
        ]
        return lax.ppermute(rows, ALL, pairs), moved

    def swap(self, rows):
        return lax.ppermute(rows, ALL, [(d, d ^ 1) for d in range(self.n_dev)])

    def others(self, piece, axis):
        size = self.shape[axis]
        found, up, down = [], piece, piece
        for _ in range((size - 1) // 2):
            up, down = self.fetch(up, axis, 1), self.fetch(down, axis, -1)
            found += [up, down]
        if size % 2 == 0 and size > 2:
            found += [self.fetch(halves(up)[0], axis, 1), self.fetch(halves(down)[1], axis, -1)]
        elif size == 2:
            found.append(self.fetch(piece, axis, 1))
        return found

    def across(self, piece):
        early, late = [], []
        for part, (first, second) in zip(halves(piece), ((1, 0), (0, 1))):
            near = self.others(part, first)
            late += self.others(joined([part] + near), second)
            early += near
        return early, late


def halves(piece):
    rows, labels = piece
    unit = rows.shape[0] // len(labels)
    cut = len(labels) // 2
    return (rows[: cut * unit], labels[:cut]), (rows[cut * unit :], labels[cut:])


def joined(pieces):
    return jnp.concatenate([p[0] for p in pieces], axis=0), sum([p[1] for p in pieces], [])


def on_device(
    expert_ids,
    expert_home,
    live_tokens,
    gate_weights,
    output_grad,
    saved_hidden,
    down_weight,
    dense_input,
    latent_grad,
):
    n_group = lax.axis_size("expert")
    n_dp = lax.axis_size("dp")
    n_dev = n_group * n_dp
    tok_rows, top_count = expert_ids.shape
    model_width = output_grad.shape[1]
    hidden_units = saved_hidden.shape[2]
    block_units = hidden_units // n_dp
    is_live = jnp.arange(tok_rows, dtype=jnp.int32) < live_tokens[0]
    masked_grad = jnp.where(is_live[:, None], latent_grad, jnp.zeros_like(latent_grad))
    torus = Torus(n_dp, n_group)
    n_core = torus.n_core
    n_y, n_x, n_z = torus.shape
    core = lax.axis_index("expert") % n_core
    place_z = lax.axis_index("expert") // n_core
    place_y = lax.axis_index("dp") // n_x
    place_x = lax.axis_index("dp") % n_x
    n_unit = 4
    unit = tok_rows // n_unit
    start = (output_grad, [(0, 0, 0, u) for u in range(n_unit)])
    near = joined([start] + torus.others(start, 2))
    id_table = expert_ids[:, :, None] == jnp.arange(expert_home.shape[0], dtype=jnp.int32)
    home_slot = jnp.sum(jnp.where(id_table, expert_home, 0), axis=2)
    pair_scale = gate_weights * is_live[:, None].astype(jnp.float32)
    chosen = home_slot[None] == jnp.arange(n_group, dtype=jnp.int32)[:, None, None]
    scaled = (saved_hidden.astype(jnp.float32) * pair_scale[:, :, None])
    spread = sum(
        jnp.where(chosen[:, :, k, None], scaled[None, :, k], jnp.float32(0.0))
        for k in range(top_count)
    ).astype(jnp.bfloat16)
    owned_width = model_width // n_dev
    latent_width = masked_grad.shape[1]
    outgoing = jnp.concatenate(
        [
            spread.reshape(n_group, tok_rows, n_dp, block_units)
            .transpose(2, 0, 1, 3)
            .reshape(n_dev, tok_rows, block_units),
            jnp.broadcast_to(masked_grad[None], (n_dev, tok_rows, latent_width)),
            dense_input.reshape(tok_rows, n_dev, owned_width).transpose(1, 0, 2),
        ],
        axis=2,
    )
    arrived = lax.all_to_all(outgoing, ALL, split_axis=0, concat_axis=0, tiled=True)
    ready, _ = lax.optimization_barrier((near[0], outgoing))
    near = (ready, near[1])
    a_rows = [(near[0][i * unit : (i + 1) * unit], [l]) for i, l in enumerate(near[1]) if l[3] < n_unit // 2]
    a_early, a_late = torus.across(joined(a_rows))
    b_early, b_late = torus.across(halves(start)[1])
    b_cross = joined(b_early + b_late)
    b_far = [b_cross] + torus.others(b_cross, 2)
    groups = [near, joined(a_early), joined(b_far), joined(a_late)]
    near_other = torus.swap(near[0])
    swapped = [near_other] + [torus.swap(g[0]) for g in groups[1:]]

    flat = arrived.reshape(n_dev * tok_rows, -1)
    dense_grad = lax.dot_general(
        flat[:, block_units + latent_width :],
        flat[:, block_units : block_units + latent_width],
        (((0,), (0,)), ((), ())),
        preferred_element_type=jnp.float32,
    )
    relative = arrived[..., :block_units].reshape(
        n_y, n_x, n_z, n_core, n_unit, unit, block_units
    )
    relative = jnp.roll(relative, -place_y, axis=0)
    relative = jnp.roll(relative, -place_x, axis=1)
    relative = jnp.roll(relative, -place_z, axis=2)
    relative = jnp.roll(relative, -core, axis=3)

    def hidden_of(labels, c):
        return jnp.concatenate([relative[y, x, z, c, u] for y, x, z, u in labels], axis=0)

    weight = down_weight[0]

    def through(rows):
        return lax.dot_general(
            rows, weight, (((1,), (1,)), ((), ())), preferred_element_type=jnp.float32
        ).astype(jnp.bfloat16)

    def in_order(rows):
        blocks = {l[2:]: rows[i * unit : (i + 1) * unit] for i, l in enumerate(near[1])}
        return jnp.stack(
            [
                jnp.concatenate([blocks[z, u] for u in range(n_unit)], axis=0)
                for z in range(n_z)
            ],
            axis=0,
        )

    part_mine = through(near[0])
    part_other = through(near_other)
    part_mine, part_other = in_order(part_mine), in_order(part_other)
    input_grad = jnp.roll(
        jnp.roll(jnp.stack([part_mine, part_other], axis=1), core, axis=1), place_z, axis=0
    )
    returned = lax.all_to_all(
        input_grad.reshape(n_group, tok_rows, hidden_units),
        "expert",
        split_axis=0,
        concat_axis=0,
        tiled=True,
    )
    over_tokens = (((0,), (0,)), ((), ()))

    def over_tokens(some):
        hidden = [hidden_of(groups[i][1], c) for c in range(n_core) for i in some]
        rows = [groups[i][0] for i in some] + [swapped[i] for i in some]
        return lax.dot_general(
            jnp.concatenate(hidden, axis=0),
            jnp.concatenate(rows, axis=0),
            (((0,), (0,)), ((), ())),
            preferred_element_type=jnp.float32,
        )

    near_sum = over_tokens([0])
    expert_grad = near_sum + over_tokens([1, 2, 3])
    picked = sum(
        jnp.where(chosen[s, :, :, None], returned[s][:, None, :].astype(jnp.float32), 0.0)
        for s in range(n_group)
    )
    hidden_grad = (picked * pair_scale[:, :, None]).astype(jnp.bfloat16)
    return (hidden_grad, expert_grad[None], dense_grad)


def solution(mesh):
    placed = (
        P(ALL, None),
        P(),
        P(ALL),
        P(ALL, None),
        P(ALL, None),
        P(ALL, None, None),
        P("expert", None, None),
        P(ALL, None),
        P(ALL, None),
    )
    return jax.shard_map(
        on_device,
        mesh=mesh,
        in_specs=placed,
        out_specs=(P(ALL, None, None), P("expert", "dp", None), P(ALL, None)),
        check_vma=False,
    )
```
